32 devices in a mesh: expert: 16 (over z, y, core), token: 2 (over x).
Axes of the slice: x: 2, y: 2, z: 4, core: 2. Of those that a mesh axis runs over, the one named last changes fastest.
Arguments:
- cotangent: bfloat16 [4096, 2048], P(('expert', 'token')), may hold values from -6 to 6
- expert_ids: int32 [4096, 6], P(('expert', 'token')), may hold values from 0 to 15, all different within a row; in each aligned block of 128 rows (0 to 127, 128 to 255, ...) at most 56 rows name the same one
- gate_values: float32 [4096, 6], P(('expert', 'token')), may hold values from 0.05 to 0.45
- hidden_pre: bfloat16 [16, 1792, 768], P('expert', 'token'), may hold values from -8 to 8
- up_weight: bfloat16 [16, 2048, 768], P('expert'), may hold values from -0.125 to 0.125
- down_weight: bfloat16 [16, 2048, 768], P('expert'), may hold values from -0.21875 to 0.21875
Outputs:
- input_grad: bfloat16 [4096, 2048], P(('expert', 'token'))
- down_grad: bfloat16 [16, 2048, 768], P('expert', 'token')
The draws below stay inside these ranges and needn't reach their ends.
Inputs may be any that keep to these rules, and one draw needn't show every extreme that they name: `expert_ids`: each row names 6 different experts. Among the 128 rows of one device no expert is named more than 56 times, and in every draw some expert is named exactly 56 times by the rows of some device.
All inputs are finite; a program needn't handle non-finite values.
Results may differ from the reference program's by a relative error of at most 0.007.
Values may be sent and summed in bfloat16 or wider, within the bound.
A program may use at most 128 MiB of HBM per device.

```python
import math
import jax
import jax.numpy as jnp
import numpy as np
from jax import lax

D = 2048
H = 768
TOP = 6
T_DEV = 128
EXPERTS = 16
CAP = 56
SLOTS = 1792
TOKENS = 4096
N_TOKEN = 2


def steps_of(rng, extent, shards, smallest, largest):
    factor_of = 1.0
    for dim, shards_of in shards:
        steps = jax.random.uniform(jax.random.fold_in(jax.random.fold_in(rng, 6), dim), (shards_of,), jnp.float32, smallest / len(shards), largest / len(shards))
        factor_of = factor_of * jnp.repeat(jnp.exp(steps), extent[dim] // shards_of).reshape((-1,) + (1,) * (len(extent) - 1 - dim))
    return factor_of


def assign_block(rng, own, number, rows, number_of, top, reach, lean):
    ranking = jax.random.permutation(rng, number_of)
    crowded, common = shares(number_of, rows * top, reach, lean, True), shares(number_of, rows * top, reach, lean, False)
    places = jnp.arange(number_of)

    def named(tallies, offset_by):
        used = int((tallies > 0).sum())
        fixed = max(1, used // 4)
        passed = fixed + (places - fixed + offset_by * (used - fixed)) % max(1, number_of - fixed)
        return jnp.zeros((number_of,), jnp.int32).at[ranking[jnp.where(places < fixed, places, passed)]].set(jnp.asarray(tallies, jnp.int32))

    tallies = jnp.where(number % 4 == 0, named(crowded, number // 4), named(common, number - number // 4 - 1))
    mixed = jax.random.permutation(jax.random.fold_in(own, 3), number_of)
    donor, receiver = mixed[0:number_of // 2 * 2:2], mixed[1:number_of // 2 * 2:2]
    margin = jnp.minimum(tallies[donor] - 1, reach - tallies[receiver]) // 2
    margin = jnp.where((donor == ranking[0]) | (receiver == ranking[0]) | (tallies[receiver] == 0), 0, jnp.maximum(margin, 0))
    passed = jax.random.randint(jax.random.fold_in(own, 4), (number_of // 2,), 0, 1 << 20) % (margin + 1)
    tallies = tallies.at[donor].add(-passed).at[receiver].add(passed)
    members = jnp.searchsorted(jnp.cumsum(tallies), jnp.arange(rows * top), side="right").astype(jnp.int32)
    listing = members.reshape(top, rows).T
    listing = listing[jax.random.permutation(jax.random.fold_in(own, 1), rows)]
    offset_by = jax.random.randint(jax.random.fold_in(own, 2), (rows, 1), 0, top)
    return jnp.take_along_axis(listing, (jnp.arange(top)[None, :] + offset_by) % top, axis=1)


def shares(amount, total, bound, lean, full):
    loads = [(1 << 20) // math.isqrt(grade ** lean) + 1 for grade in range(1, amount + 1)]
    largest = bound if full else min(bound, max(-(-total // amount), total * loads[0] // sum(loads)))
    least = 1 if total - largest >= amount - 1 else 0
    holding, rest = [largest] + [least] * (amount - 1), total - largest - least * (amount - 1)
    while rest > 0:
        free = [i for i in range(1, amount) if holding[i] < largest] or [i for i in range(1, amount) if holding[i] < bound]
        pool, budget = sum([loads[i] for i in free]), rest
        for i in free:
            addition = min(bound - holding[i], max(1, budget * loads[i] // pool), rest)
            holding[i] = holding[i] + addition
            rest = rest - addition
    return np.array(holding)


def scatter_about(rng, dims, scale, bound, split=(), kind=jnp.bfloat16):
    factor_of = steps_of(rng, dims, split, -0.22, 0.18) if split else 1.0
    values = jax.random.normal(rng, dims, jnp.float32) * scale * factor_of
    return jnp.minimum(jnp.maximum(values, -bound), bound).astype(kind)


def setup_inputs(seed: int = 0) -> dict:
    splits = jax.random.split(jax.random.key(seed), 7)
    cotangent = scatter_about(splits[0], (TOKENS, D), 1.0, 6.0, ((0, 32),))
    expert_ids_keys = jax.random.split(jax.random.fold_in(splits[1], 1), TOKENS // T_DEV)
    expert_ids_turns = jax.random.permutation(jax.random.fold_in(splits[1], 3), TOKENS // T_DEV)
    expert_ids = jax.vmap(lambda own, number: assign_block(jax.random.fold_in(splits[1], 2), own, number, T_DEV, EXPERTS, TOP, CAP, 2))(expert_ids_keys, expert_ids_turns).reshape((TOKENS, TOP))
    gate_values = jnp.clip(0.05 + 0.39999999 * jax.random.uniform(splits[2], (TOKENS, TOP), jnp.float32) ** steps_of(splits[2], (TOKENS, TOP), ((0, 32),), -0.2, 0.2), 0.05, 0.45)
    hidden_pre = scatter_about(splits[3], (EXPERTS, SLOTS, H), 1.5, 8.0, ((0, 16), (1, 2)))
    up_weight = scatter_about(splits[4], (EXPERTS, D, H), D ** -0.5, 0.125, ((0, 16),))
    down_weight = scatter_about(splits[5], (EXPERTS, D, H), H ** -0.5, 0.21875, ((0, 16),))
    return {"cotangent": cotangent, "expert_ids": expert_ids, "gate_values": gate_values, "hidden_pre": hidden_pre, "up_weight": up_weight, "down_weight": down_weight}


grad_scale = 0.03125
root_half = 0.7071067811865476
inv_root_two_pi = 0.3989422804014327


def slope_and_act(hidden_rows):
    values = hidden_rows.astype(jnp.float32)
    normal_cdf = 0.5 * (1.0 + lax.erf(values * root_half))
    density = inv_root_two_pi * jnp.exp(-0.5 * values * values)
    slopes = normal_cdf + values * density
    active = (values * normal_cdf).astype(jnp.bfloat16)
    return slopes, active


def slot_tables(expert_ids, gate_values, slot_count):
    top_count = expert_ids.shape[1]
    blocks = expert_ids.shape[0] // T_DEV
    grouped = expert_ids.reshape(blocks, T_DEV * top_count)
    one_hot = (grouped[:, :, None] == jnp.arange(EXPERTS, dtype=jnp.int32)[None, None, :]).astype(jnp.int32)
    earlier = jnp.cumsum(one_hot, axis=1) - one_hot
    rank_in = jnp.sum(earlier * one_hot, axis=2).astype(jnp.int32)
    block_ids = jnp.arange(blocks, dtype=jnp.int32)[:, None]
    slot_row = (block_ids % N_TOKEN) * (EXPERTS * CAP) + (block_ids // N_TOKEN) * CAP + rank_in
    token_ids = block_ids * T_DEV + jnp.arange(T_DEV * top_count, dtype=jnp.int32)[None, :] // top_count
    flat_expert = grouped.reshape(-1).astype(jnp.int32)
    flat_slot = slot_row.reshape(-1).astype(jnp.int32)
    slot_token = jnp.zeros((EXPERTS, slot_count), jnp.int32).at[flat_expert, flat_slot].set(token_ids.reshape(-1).astype(jnp.int32))
    slot_gate = jnp.zeros((EXPERTS, slot_count), jnp.float32).at[flat_expert, flat_slot].set(gate_values.reshape(-1))
    slot_live = jnp.zeros((EXPERTS, slot_count), jnp.float32).at[flat_expert, flat_slot].set(jnp.ones_like(gate_values.reshape(-1)))
    return slot_token, slot_gate, slot_live


def apply_transpose(token_rows, slot_token, slot_gate, slot_live, hidden_pre, up_weight, down_weight):
    def per_expert(summed, stacked):
        token_ids, gate_e, live_e, hidden_e, up_e, down_e = stacked
        slopes, unused_act = slope_and_act(hidden_e)
        gathered = jnp.take(token_rows, token_ids, axis=0)
        gathered = jnp.where(live_e[:, None] > 0.5, gathered, jnp.zeros_like(gathered))
        inner_prod = jnp.dot(gathered, down_e, preferred_element_type=jnp.float32)
        scaled = (inner_prod * slopes).astype(jnp.bfloat16)
        pieces = jnp.dot(scaled, up_e.T, preferred_element_type=jnp.float32).astype(jnp.bfloat16)
        weighted = pieces.astype(jnp.float32) * gate_e[:, None]
        summed = summed.at[token_ids].add(weighted)
        return summed, jnp.zeros((), jnp.float32)

    initial = jnp.zeros(token_rows.shape, jnp.float32)
    summed, unused_out = lax.scan(per_expert, initial, (slot_token, slot_gate, slot_live, hidden_pre, up_weight, down_weight))
    return summed.astype(jnp.bfloat16)


def reference(cotangent, expert_ids, gate_values, hidden_pre, up_weight, down_weight):
    slot_token, slot_gate, slot_live = slot_tables(expert_ids, gate_values, hidden_pre.shape[1])
    first_term = apply_transpose(cotangent, slot_token, slot_gate, slot_live, hidden_pre, up_weight, down_weight)
    second = apply_transpose(first_term, slot_token, slot_gate, slot_live, hidden_pre, up_weight, down_weight)
    input_grad = (cotangent.astype(jnp.float32) + first_term.astype(jnp.float32) + second.astype(jnp.float32)).astype(jnp.bfloat16)

    def grad_expert(carried, stacked):
        token_ids, gate_e, hidden_e = stacked
        unused_slope, active = slope_and_act(hidden_e)
        picked = jnp.take(input_grad, token_ids, axis=0).astype(jnp.float32)
        routed = (picked * gate_e[:, None]).astype(jnp.bfloat16)
        grad_e = jnp.dot(routed.T, active, preferred_element_type=jnp.float32)
        return carried, (grad_e * grad_scale).astype(jnp.bfloat16)

    unused_carry, down_grad = lax.scan(grad_expert, jnp.zeros((), jnp.float32), (slot_token, slot_gate, hidden_pre))
    return input_grad, down_grad
```

```python
import jax
import jax.numpy as jnp
from jax import lax
from jax.sharding import PartitionSpec as P

grad_scale = 0.03125
root_half = 0.7071067811865476
inv_root_two_pi = 0.3989422804014327


def slope_and_act(hidden_rows):
    values = hidden_rows.astype(jnp.float32)
    normal_cdf = 0.5 * (1.0 + lax.erf(values * root_half))
    density = inv_root_two_pi * jnp.exp(-0.5 * values * values)
    slopes = normal_cdf + values * density
    active = (values * normal_cdf).astype(jnp.bfloat16)
    return (slopes, active)


def slot_tables(ids, gates, capacity):
    me = lax.axis_index("expert")
    hit = ids == me
    match = jnp.any(hit, axis=2)
    gate = jnp.sum(jnp.where(hit, gates, 0.0), axis=2)
    rows = ids.shape[1]
    order = jnp.arange(rows, dtype=jnp.int32)
    before = (order[:, None] < order[None, :]).astype(jnp.bfloat16)
    rank = jnp.dot(match.astype(jnp.bfloat16), before, preferred_element_type=jnp.float32)
    rank = jnp.where(match, rank.astype(jnp.int32), -1)
    chosen = rank[:, None, :] == jnp.arange(capacity, dtype=jnp.int32)[None, :, None]
    slot_gate = jnp.sum(jnp.where(chosen, gate[:, None, :], 0.0), axis=2)
    return chosen.astype(jnp.bfloat16), slot_gate


def gather_rows(rows):
    return lax.all_gather(rows, "expert", axis=0, tiled=False)


def scatter_sum(blocks):
    return lax.psum_scatter(blocks, "expert", scatter_dimension=0, tiled=False)


def pick(sel, rows):
    return lax.dot_general(
        sel, rows, (((2,), (1,)), ((0,), (0,))), preferred_element_type=jnp.float32
    ).astype(jnp.bfloat16)


def transpose_jacobian(token_rows, sel, slot_gate, slopes, up_weight, down_weight):
    blocks, capacity, rows = sel.shape
    everyone = gather_rows(token_rows)
    picked = pick(sel, everyone).reshape(blocks * capacity, -1)
    inner_prod = jnp.dot(picked, down_weight, preferred_element_type=jnp.float32)
    scaled = (inner_prod * slopes).astype(jnp.bfloat16)
    pieces = lax.dot_general(
        scaled, up_weight, (((1,), (1,)), ((), ())), preferred_element_type=jnp.float32
    ).astype(jnp.bfloat16)
    weighted = (pieces.astype(jnp.float32) * slot_gate.reshape(-1, 1)).astype(jnp.bfloat16)
    spread = lax.dot_general(
        sel,
        weighted.reshape(blocks, capacity, -1),
        (((1,), (1,)), ((0,), (0,))),
        preferred_element_type=jnp.float32,
    ).astype(jnp.bfloat16)
    return scatter_sum(spread)


def body(cotangent, expert_ids, gate_values, hidden_pre, up_weight, down_weight):
    experts = lax.axis_size("expert")
    groups = lax.axis_size("token")
    mine = lax.axis_index("token")
    slopes, active = slope_and_act(hidden_pre[0])
    capacity = slopes.shape[0] // experts
    both_ids = lax.all_gather(expert_ids, ("expert", "token"), axis=0, tiled=False)
    both_gates = lax.all_gather(gate_values, ("expert", "token"), axis=0, tiled=False)
    all_sel, all_gate = slot_tables(both_ids, both_gates, capacity)
    all_sel = all_sel.reshape(experts, groups, capacity, -1)
    all_gate = all_gate.reshape(experts, groups, capacity)
    sel = lax.dynamic_index_in_dim(all_sel, mine, 1, keepdims=False)
    slot_gate = lax.dynamic_index_in_dim(all_gate, mine, 1, keepdims=False)
    first_term = transpose_jacobian(
        cotangent, sel, slot_gate, slopes, up_weight[0], down_weight[0]
    )
    second = transpose_jacobian(
        first_term, sel, slot_gate, slopes, up_weight[0], down_weight[0]
    )
    input_grad = (
        cotangent.astype(jnp.float32) + first_term.astype(jnp.float32) + second.astype(jnp.float32)
    ).astype(jnp.bfloat16)
    rows = input_grad.shape[0]
    columns = lax.all_to_all(input_grad, "token", split_axis=1, concat_axis=0, tiled=True)
    everyone = gather_rows(columns).reshape(experts * groups, rows, -1)
    picked = pick(all_sel.reshape(experts * groups, capacity, rows), everyone)
    routed = (picked.astype(jnp.float32) * all_gate.reshape(-1, capacity, 1)).astype(jnp.bfloat16)
    acts = lax.all_gather(active, "token", axis=0, tiled=False)
    acts = acts.reshape(groups, experts, capacity, -1).transpose(1, 0, 2, 3)
    summed = lax.dot_general(
        routed.reshape(experts * groups * capacity, -1),
        acts.reshape(experts * groups * capacity, -1),
        (((0,), (0,)), ((), ())),
        preferred_element_type=jnp.float32,
    )
    grad_out = (summed * grad_scale).astype(jnp.bfloat16)[None]
    return (input_grad, grad_out)


def solution(mesh):
    in_specs = (
        P(("expert", "token"), None),
        P(("expert", "token"), None),
        P(("expert", "token"), None),
        P("expert", "token", None),
        P("expert", None, None),
        P("expert", None, None),
    )
    out_specs = (P(("expert", "token"), None), P("expert", "token", None))
    return jax.shard_map(body, mesh=mesh, in_specs=in_specs, out_specs=out_specs, check_vma=False)
```

```python
import functools

import jax
import jax.numpy as jnp
from jax import lax
from jax.experimental import pallas as pl
from jax.experimental.pallas import tpu as pltpu
from jax.sharding import PartitionSpec as P

grad_scale = 0.03125
root_half = 0.7071067811865476
inv_root_two_pi = 0.3989422804014327


def slope_and_act(hidden_rows):
    values = hidden_rows.astype(jnp.float32)
    normal_cdf = 0.5 * (1.0 + lax.erf(values * root_half))
    density = inv_root_two_pi * jnp.exp(-0.5 * values * values)
    slopes = normal_cdf + values * density
    active = (values * normal_cdf).astype(jnp.bfloat16)
    return (slopes, active)


def slot_tables(ids, gates, capacity):
    me = lax.axis_index("expert")
    hit = ids == me
    match = jnp.any(hit, axis=2)
    gate = jnp.sum(jnp.where(hit, gates, 0.0), axis=2)
    rows = ids.shape[1]
    order = jnp.arange(rows, dtype=jnp.int32)
    before = (order[:, None] < order[None, :]).astype(jnp.bfloat16)
    rank = jnp.dot(match.astype(jnp.bfloat16), before, preferred_element_type=jnp.float32)
    rank = jnp.where(match, rank.astype(jnp.int32), -1)
    chosen = rank[:, None, :] == jnp.arange(capacity, dtype=jnp.int32)[None, :, None]
    slot_gate = jnp.sum(jnp.where(chosen, gate[:, None, :], 0.0), axis=2)
    return chosen.astype(jnp.bfloat16), slot_gate


MESH = pl.DeviceIdType.MESH


def ring_place(experts):
    chips = experts // 2
    side = chips // 2
    me = lax.axis_index("expert")
    core = me % 2
    chip = me // 2
    row, odd = chip // 2, chip % 2
    place = row + odd * (chips - 1 - 2 * row)

    def device(at):
        at = (at + 2 * chips) % chips
        back = at // side
        return ((at + back * (chips - 1 - 2 * at)) * 2 + back) * 2

    return place, core, device


def ring_messages(chips):
    side = chips // 2
    return [
        [(d, h) for d in range(1, side + 1) for h in range(2) if d < side or h == way]
        for way in range(2)
    ]


def greet(peers):
    barrier = pltpu.get_barrier_semaphore()
    for peer in peers:
        pl.semaphore_signal(barrier, inc=1, device_id={"expert": peer}, device_id_type=MESH)
    pl.semaphore_wait(barrier, len(peers))


def send(src, dst, send_sem, recv_sem, peer):
    return pltpu.make_async_remote_copy(
        src_ref=src,
        dst_ref=dst,
        send_sem=send_sem,
        recv_sem=recv_sem,
        device_id={"expert": peer},
        device_id_type=MESH,
    )


def gather_kernel(experts, count, *refs):
    mine, outs = refs[:count], refs[count : 2 * count]
    hop_send, hop_recv, sib_send, sib_recv, own_sem, cross_sems = refs[2 * count :]
    chips = experts // 2
    messages = ring_messages(chips)
    place, core, device = ring_place(experts)
    me = lax.axis_index("expert")
    sibling = me + 1 - 2 * core
    peers = (device(place + 1) + core, device(place - 1) + core)
    own = [pltpu.make_async_copy(mine[i], outs[i].at[me], own_sem.at[i]) for i in range(count)]
    for copy in own:
        copy.start()
    greet(peers + (sibling,))

    def rows_of(i, half):
        size = mine[i].shape[0] // 2
        return pl.ds(half * size, size)

    def hop(i, way, index):
        distance, half = messages[way][index]
        sign = 1 - 2 * way
        rows = rows_of(i, half)
        origin = device(place - sign * (distance - 1)) + core
        src = mine[i].at[rows] if distance == 1 else outs[i].at[origin, rows]
        return send(
            src,
            outs[i].at[origin, rows],
            hop_send.at[i, way, index],
            hop_recv.at[i, way, index],
            peers[way],
        )

    def landed(i, way, index, which):
        distance, half = messages[way][index]
        origin = device(place - (1 - 2 * way) * distance) + which
        return outs[i].at[origin, rows_of(i, half)]

    def across(i, way, index, which):
        block = landed(i, way, index, which)
        return send(
            block, block, sib_send.at[i, way, index], sib_recv.at[i, way, index], sibling
        )

    for index in range(2):
        for way in range(2):
            for i in range(count):
                if index < len(messages[way]) and messages[way][index][0] == 1:
                    hop(i, way, index).start()
    cross = [
        send(mine[i], outs[i].at[me], cross_sems.at[0, i], cross_sems.at[1, i], sibling)
        for i in range(count)
    ]
    for copy in cross:
        copy.start()
    for index in range(len(messages[0])):
        for way in range(2):
            distance, half = messages[way][index]
            for i in range(count):
                block = landed(i, way, index, core)
                send(
                    block,
                    block,
                    hop_send.at[i, way, index],
                    hop_recv.at[i, way, index],
                    peers[way],
                ).wait_recv()
                if (distance + 1, half) in messages[way]:
                    hop(i, way, messages[way].index((distance + 1, half))).start()
                across(i, way, index, core).start()
    for i in range(count):
        own[i].wait()
        cross[i].wait_send()
        send(
            mine[i], outs[i].at[sibling], cross_sems.at[0, i], cross_sems.at[1, i], sibling
        ).wait_recv()
        for way in range(2):
            for index in range(len(messages[way])):
                hop(i, way, index).wait_send()
                across(i, way, index, core).wait_send()
                across(i, way, index, 1 - core).wait_recv()


def gather_rows(arrays, name):
    experts = lax.axis_size("expert")
    count = len(arrays)
    steps = len(ring_messages(experts // 2)[0])
    dma = pltpu.SemaphoreType.DMA
    return pl.pallas_call(
        functools.partial(gather_kernel, experts, count),
        out_shape=[jax.ShapeDtypeStruct((experts,) + a.shape, a.dtype) for a in arrays],
        in_specs=[pl.BlockSpec(memory_space=pltpu.VMEM)] * count,
        out_specs=[pl.BlockSpec(memory_space=pl.ANY)] * count,
        scratch_shapes=[
            dma((count, 2, steps)),
            dma((count, 2, steps)),
            dma((count, 2, steps)),
            dma((count, 2, steps)),
            dma((count,)),
            dma((2, count)),
        ],
        compiler_params=pltpu.CompilerParams(
            collective_id=name, has_side_effects=True, vmem_limit_bytes=8 * 1024 * 1024
        ),
        cost_estimate=pl.CostEstimate(
            flops=20_000_000_000, bytes_accessed=20_000_000, transcendentals=0
        ),
        name="gather" + str(name),
    )(*arrays)


def scatter_kernel(
    experts, parts, out, own, other, came, own_sem, sib_send, sib_recv, hop_send, hop_recv
):
    chips = experts // 2
    side = chips // 2
    messages = ring_messages(chips)
    place, core, device = ring_place(experts)
    me = lax.axis_index("expert")
    sibling = me + 1 - 2 * core
    peers = (device(place + 1) + core, device(place - 1) + core)
    size = out.shape[0] // 2
    order = [side]
    for d in range(side - 1, 0, -1):
        order += [d, chips - d]
    order += [0]
    loads = {
        k: pltpu.make_async_copy(parts.at[device(place + k) + core], own.at[k], own_sem.at[k])
        for k in order
    }
    for k in order:
        loads[k].start()
    greet(peers + (sibling,))
    gifts = {
        k: send(
            parts.at[device(place + k) + 1 - core],
            other.at[k],
            sib_send.at[k],
            sib_recv.at[k],
            sibling,
        )
        for k in order
    }
    for k in order:
        gifts[k].start()

    def hop(way, message):
        distance, half = message
        k = distance if way == 0 else chips - distance
        rows = pl.ds(half * size, size)
        index = messages[way].index(message)
        return send(
            own.at[k, rows],
            came.at[way, distance - 1, rows],
            hop_send.at[way, index],
            hop_recv.at[way, index],
            peers[way],
        )

    step = 16

    def add_up(k, half, more, target):
        @pl.loop(0, size // step)
        def _(at):
            rows = pl.ds(pl.multiple_of(half * size + at * step, step), step)
            total = own[k, rows, :].astype(jnp.float32) + other[k, rows, :].astype(jnp.float32)
            for way, slot in more:
                total = total + came[way, slot, rows, :].astype(jnp.float32)
            if target is None:
                own[k, rows, :] = total.astype(own.dtype)
            else:
                target[rows, :] = total.astype(target.dtype)

    ready = set()

    def get(k):
        if k not in ready:
            ready.add(k)
            loads[k].wait()
            gifts[k].wait_recv()

    for distance in range(side, 0, -1):
        for half in range(2):
            for way in range(2):
                if (distance, half) not in messages[way]:
                    continue
                k = distance if way == 0 else chips - distance
                get(k)
                more = []
                if (distance + 1, half) in messages[way]:
                    hop(way, (distance + 1, half)).wait_recv()
                    more = [(way, distance)]
                add_up(k, half, more, None)
                hop(way, (distance, half)).start()
    get(0)
    for half in range(2):
        more = []
        for way in range(2):
            if (1, half) in messages[way]:
                hop(way, (1, half)).wait_recv()
                more.append((way, 0))
        add_up(0, half, more, out)
    for k in order:
        gifts[k].wait_send()
    for way in range(2):
        for message in messages[way]:
            hop(way, message).wait_send()


def scatter_sum(blocks):
    experts, rows, width = blocks.shape
    chips = experts // 2
    steps = len(ring_messages(chips)[0])
    dma = pltpu.SemaphoreType.DMA
    buffers = (3 * chips + 4) * rows * width * 2
    return pl.pallas_call(
        functools.partial(scatter_kernel, experts),
        out_shape=jax.ShapeDtypeStruct((rows, width), blocks.dtype),
        in_specs=[pl.BlockSpec(memory_space=pl.ANY)],
        out_specs=pl.BlockSpec(memory_space=pltpu.VMEM),
        scratch_shapes=[
            pltpu.VMEM((chips, rows, width), blocks.dtype),
            pltpu.VMEM((chips, rows, width), blocks.dtype),
            pltpu.VMEM((2, chips // 2, rows, width), blocks.dtype),
            dma((chips,)),
            dma((chips,)),
            dma((chips,)),
            dma((2, steps)),
            dma((2, steps)),
        ],
        compiler_params=pltpu.CompilerParams(
            collective_id=7, has_side_effects=True, vmem_limit_bytes=buffers + 2 * 1024 * 1024
        ),
        cost_estimate=pl.CostEstimate(
            flops=20_000_000_000, bytes_accessed=20_000_000, transcendentals=0
        ),
        name="scatter_sum",
    )(blocks)


def from_groups(make):
    groups = lax.axis_size("token")
    mine = lax.axis_index("token")
    taken = [make(mine)]
    for shift in range(1, groups):
        pairs = [(t, (t + shift) % groups) for t in range(groups)]
        taken.append(lax.ppermute(make((mine + shift) % groups), "token", pairs))
    return jnp.stack(taken)


def pick(sel, rows):
    return lax.dot_general(
        sel, rows, (((2,), (1,)), ((0,), (0,))), preferred_element_type=jnp.float32
    ).astype(jnp.bfloat16)


def transpose_jacobian(everyone, sel, slot_gate, slopes, up_weight, down_weight):
    blocks, capacity, rows = sel.shape
    picked = pick(sel, everyone).reshape(blocks * capacity, -1)
    inner_prod = jnp.dot(picked, down_weight, preferred_element_type=jnp.float32)
    scaled = (inner_prod * slopes).astype(jnp.bfloat16)
    pieces = lax.dot_general(
        scaled, up_weight, (((1,), (1,)), ((), ())), preferred_element_type=jnp.float32
    ).astype(jnp.bfloat16)
    weighted = (pieces.astype(jnp.float32) * slot_gate.reshape(-1, 1)).astype(jnp.bfloat16)
    spread = lax.dot_general(
        sel,
        weighted.reshape(blocks, capacity, -1),
        (((1,), (1,)), ((0,), (0,))),
        preferred_element_type=jnp.float32,
    ).astype(jnp.bfloat16)
    return scatter_sum(spread)


def body(cotangent, expert_ids, gate_values, hidden_pre, up_weight, down_weight):
    experts = lax.axis_size("expert")
    groups = lax.axis_size("token")
    rows, width = cotangent.shape
    top = expert_ids.shape[1]
    padded = -(-2 * top // 16) * 16
    routes = jnp.concatenate([expert_ids.T.astype(jnp.float32), gate_values.T], axis=0)
    routes = jnp.pad(routes, ((0, padded - 2 * top), (0, 0)))
    routes = from_groups(lambda group: routes).reshape(groups * padded, rows)
    everyone, all_routes = gather_rows([cotangent, routes], 1)
    slopes, active = slope_and_act(hidden_pre[0])
    capacity = slopes.shape[0] // experts
    acts = from_groups(lambda group: active)
    all_routes = all_routes.reshape(experts * groups, padded, rows).transpose(0, 2, 1)
    all_sel, all_gate = slot_tables(
        all_routes[:, :, :top].astype(jnp.int32), all_routes[:, :, top : 2 * top], capacity
    )
    by_group = all_sel.reshape(experts, groups, capacity, rows)
    sel = by_group[:, 0]
    slot_gate = all_gate.reshape(experts, groups, capacity)[:, 0]
    first_term = transpose_jacobian(
        everyone, sel, slot_gate, slopes, up_weight[0], down_weight[0]
    )
    (everyone,) = gather_rows([first_term], 2)
    second = transpose_jacobian(everyone, sel, slot_gate, slopes, up_weight[0], down_weight[0])
    input_grad = (
        cotangent.astype(jnp.float32) + first_term.astype(jnp.float32) + second.astype(jnp.float32)
    ).astype(jnp.bfloat16)
    share = width // groups
    columns = from_groups(
        lambda group: lax.dynamic_slice_in_dim(input_grad, group * share, share, 1)
    ).reshape(groups * rows, share)
    (everyone,) = gather_rows([columns], 3)
    everyone = everyone.reshape(experts * groups, rows, share)
    picked = pick(all_sel, everyone)
    routed = (picked.astype(jnp.float32) * all_gate[:, :, None]).astype(jnp.bfloat16)
    acts = acts.reshape(groups, experts, capacity, -1).transpose(1, 0, 2, 3)
    summed = lax.dot_general(
        routed.reshape(experts * groups * capacity, -1),
        acts.reshape(experts * groups * capacity, -1),
        (((0,), (0,)), ((), ())),
        preferred_element_type=jnp.float32,
    )
    grad_out = (summed * grad_scale).astype(jnp.bfloat16)[None]
    return (input_grad, grad_out)


def solution(mesh):
    in_specs = (
        P(("expert", "token"), None),
        P(("expert", "token"), None),
        P(("expert", "token"), None),
        P("expert", "token", None),
        P("expert", None, None),
        P("expert", None, None),
    )
    out_specs = (P(("expert", "token"), None), P("expert", "token", None))
    return jax.shard_map(body, mesh=mesh, in_specs=in_specs, out_specs=out_specs, check_vma=False)
```

```python
import functools

import jax
import jax.numpy as jnp
from jax import lax
from jax.experimental import pallas as pl
from jax.experimental.pallas import tpu as pltpu
from jax.sharding import PartitionSpec as P

grad_scale = 0.03125
root_half = 0.7071067811865476
inv_root_two_pi = 0.3989422804014327


def slope_and_act(hidden_rows):
    values = hidden_rows.astype(jnp.float32)
    normal_cdf = 0.5 * (1.0 + lax.erf(values * root_half))
    density = inv_root_two_pi * jnp.exp(-0.5 * values * values)
    slopes = normal_cdf + values * density
    active = (values * normal_cdf).astype(jnp.bfloat16)
    return (slopes, active)


def slot_tables(ids, gates, capacity):
    me = lax.axis_index("expert")
    hit = ids == me
    match = jnp.any(hit, axis=2)
    gate = jnp.sum(jnp.where(hit, gates, 0.0), axis=2)
    rows = ids.shape[1]
    order = jnp.arange(rows, dtype=jnp.int32)
    before = (order[:, None] < order[None, :]).astype(jnp.bfloat16)
    rank = jnp.dot(match.astype(jnp.bfloat16), before, preferred_element_type=jnp.float32)
    rank = jnp.where(match, rank.astype(jnp.int32), -1)
    chosen = rank[:, None, :] == jnp.arange(capacity, dtype=jnp.int32)[None, :, None]
    slot_gate = jnp.sum(jnp.where(chosen, gate[:, None, :], 0.0), axis=2)
    return chosen.astype(jnp.bfloat16), slot_gate


MESH = pl.DeviceIdType.MESH


def ring_place(experts):
    chips = experts // 2
    side = chips // 2
    me = lax.axis_index("expert")
    core = me % 2
    chip = me // 2
    row, odd = chip // 2, chip % 2
    place = row + odd * (chips - 1 - 2 * row)

    def device(at):
        at = (at + 2 * chips) % chips
        back = at // side
        return ((at + back * (chips - 1 - 2 * at)) * 2 + back) * 2

    return place, core, device


def ring_messages(chips):
    side = chips // 2
    return [
        [(d, h) for d in range(1, side + 1) for h in range(2) if d < side or h == way]
        for way in range(2)
    ]


def greet(peers):
    barrier = pltpu.get_barrier_semaphore()
    for peer in peers:
        pl.semaphore_signal(barrier, inc=1, device_id={"expert": peer}, device_id_type=MESH)
    pl.semaphore_wait(barrier, len(peers))


def send(src, dst, send_sem, recv_sem, peer):
    return pltpu.make_async_remote_copy(
        src_ref=src,
        dst_ref=dst,
        send_sem=send_sem,
        recv_sem=recv_sem,
        device_id={"expert": peer},
        device_id_type=MESH,
    )


def gather_kernel(experts, count, *refs):
    hop_send, hop_recv, sib_send, sib_recv, own_sem, cross_sems = refs[-6:]
    mine, refs = refs[:count], refs[count:-6]
    hidden = refs[: (len(refs) - count) // 3]
    outs = refs[len(hidden) : len(hidden) + count]
    chips = experts // 2
    messages = ring_messages(chips)
    place, core, device = ring_place(experts)
    me = lax.axis_index("expert")
    sibling = me + 1 - 2 * core
    peers = (device(place + 1) + core, device(place - 1) + core)
    own = [pltpu.make_async_copy(mine[i], outs[i].at[me], own_sem.at[i]) for i in range(count)]
    for copy in own:
        copy.start()
    greet(peers + (sibling,))

    def rows_of(i, half):
        size = mine[i].shape[0] // 2
        return pl.ds(half * size, size)

    def hop(i, way, index):
        distance, half = messages[way][index]
        sign = 1 - 2 * way
        rows = rows_of(i, half)
        origin = device(place - sign * (distance - 1)) + core
        src = mine[i].at[rows] if distance == 1 else outs[i].at[origin, rows]
        return send(
            src,
            outs[i].at[origin, rows],
            hop_send.at[i, way, index],
            hop_recv.at[i, way, index],
            peers[way],
        )

    def landed(i, way, index, which):
        distance, half = messages[way][index]
        origin = device(place - (1 - 2 * way) * distance) + which
        return outs[i].at[origin, rows_of(i, half)]

    def across(i, way, index, which):
        block = landed(i, way, index, which)
        return send(
            block, block, sib_send.at[i, way, index], sib_recv.at[i, way, index], sibling
        )

    for index in range(2):
        for way in range(2):
            for i in range(count):
                if index < len(messages[way]) and messages[way][index][0] == 1:
                    hop(i, way, index).start()
    cross = [
        send(mine[i], outs[i].at[me], cross_sems.at[0, i], cross_sems.at[1, i], sibling)
        for i in range(count)
    ]
    for copy in cross:
        copy.start()
    if hidden:
        (hidden_ref,), (slope_ref, act_ref) = hidden, refs[1 + count :]
        step = 16

        @pl.loop(0, hidden_ref.shape[0] // step)
        def _(at):
            rows = pl.ds(pl.multiple_of(at * step, step), step)
            slope_ref[rows, :], act_ref[rows, :] = slope_and_act(hidden_ref[rows, :])

    for index in range(len(messages[0])):
        for way in range(2):
            distance, half = messages[way][index]
            for i in range(count):
                block = landed(i, way, index, core)
                send(
                    block,
                    block,
                    hop_send.at[i, way, index],
                    hop_recv.at[i, way, index],
                    peers[way],
                ).wait_recv()
                if (distance + 1, half) in messages[way]:
                    hop(i, way, messages[way].index((distance + 1, half))).start()
                across(i, way, index, core).start()
    for i in range(count):
        own[i].wait()
        cross[i].wait_send()
        send(
            mine[i], outs[i].at[sibling], cross_sems.at[0, i], cross_sems.at[1, i], sibling
        ).wait_recv()
        for way in range(2):
            for index in range(len(messages[way])):
                hop(i, way, index).wait_send()
                across(i, way, index, core).wait_send()
                across(i, way, index, 1 - core).wait_recv()


def gather_rows(arrays, name, hidden=()):
    experts = lax.axis_size("expert")
    count = len(arrays)
    steps = len(ring_messages(experts // 2)[0])
    dma = pltpu.SemaphoreType.DMA
    return pl.pallas_call(
        functools.partial(gather_kernel, experts, count),
        out_shape=[jax.ShapeDtypeStruct((experts,) + a.shape, a.dtype) for a in arrays]
        + [jax.ShapeDtypeStruct(a.shape, kind) for a in hidden for kind in (jnp.float32, a.dtype)],
        in_specs=[pl.BlockSpec(memory_space=pltpu.VMEM)] * (count + len(hidden)),
        out_specs=[pl.BlockSpec(memory_space=pl.ANY)] * count
        + [pl.BlockSpec(memory_space=pltpu.VMEM)] * (2 * len(hidden)),
        scratch_shapes=[
            dma((count, 2, steps)),
            dma((count, 2, steps)),
            dma((count, 2, steps)),
            dma((count, 2, steps)),
            dma((count,)),
            dma((2, count)),
        ],
        compiler_params=pltpu.CompilerParams(
            collective_id=name, has_side_effects=True, vmem_limit_bytes=(16 if hidden else 8) * 1024 * 1024
        ),
        cost_estimate=pl.CostEstimate(
            flops=20_000_000_000, bytes_accessed=20_000_000, transcendentals=0
        ),
        name="gather" + str(name),
    )(*arrays, *hidden)


def scatter_kernel(
    experts, parts, out, own, other, came, own_sem, sib_send, sib_recv, hop_send, hop_recv
):
    chips = experts // 2
    side = chips // 2
    messages = ring_messages(chips)
    place, core, device = ring_place(experts)
    me = lax.axis_index("expert")
    sibling = me + 1 - 2 * core
    peers = (device(place + 1) + core, device(place - 1) + core)
    size = out.shape[0] // 2
    order = [side]
    for d in range(side - 1, 0, -1):
        order += [d, chips - d]
    order += [0]
    loads = {
        k: pltpu.make_async_copy(parts.at[device(place + k) + core], own.at[k], own_sem.at[k])
        for k in order
    }
    for k in order:
        loads[k].start()
    greet(peers + (sibling,))
    gifts = {
        k: send(
            parts.at[device(place + k) + 1 - core],
            other.at[k],
            sib_send.at[k],
            sib_recv.at[k],
            sibling,
        )
        for k in order
    }
    for k in order:
        gifts[k].start()

    def hop(way, message):
        distance, half = message
        k = distance if way == 0 else chips - distance
        rows = pl.ds(half * size, size)
        index = messages[way].index(message)
        return send(
            own.at[k, rows],
            came.at[way, distance - 1, rows],
            hop_send.at[way, index],
            hop_recv.at[way, index],
            peers[way],
        )

    step = 16

    def add_up(k, half, more, target):
        @pl.loop(0, size // step)
        def _(at):
            rows = pl.ds(pl.multiple_of(half * size + at * step, step), step)
            total = own[k, rows, :].astype(jnp.float32) + other[k, rows, :].astype(jnp.float32)
            for way, slot in more:
                total = total + came[way, slot, rows, :].astype(jnp.float32)
            if target is None:
                own[k, rows, :] = total.astype(own.dtype)
            else:
                target[rows, :] = total.astype(target.dtype)

    ready = set()

    def get(k):
        if k not in ready:
            ready.add(k)
            loads[k].wait()
            gifts[k].wait_recv()

    for distance in range(side, 0, -1):
        for half in range(2):
            for way in range(2):
                if (distance, half) not in messages[way]:
                    continue
                k = distance if way == 0 else chips - distance
                get(k)
                more = []
                if (distance + 1, half) in messages[way]:
                    hop(way, (distance + 1, half)).wait_recv()
                    more = [(way, distance)]
                add_up(k, half, more, None)
                hop(way, (distance, half)).start()
    get(0)
    for half in range(2):
        more = []
        for way in range(2):
            if (1, half) in messages[way]:
                hop(way, (1, half)).wait_recv()
                more.append((way, 0))
        add_up(0, half, more, out)
    for k in order:
        gifts[k].wait_send()
    for way in range(2):
        for message in messages[way]:
            hop(way, message).wait_send()


def scatter_sum(blocks):
    experts, rows, width = blocks.shape
    chips = experts // 2
    steps = len(ring_messages(chips)[0])
    dma = pltpu.SemaphoreType.DMA
    buffers = (3 * chips + 4) * rows * width * 2
    return pl.pallas_call(
        functools.partial(scatter_kernel, experts),
        out_shape=jax.ShapeDtypeStruct((rows, width), blocks.dtype),
        in_specs=[pl.BlockSpec(memory_space=pl.ANY)],
        out_specs=pl.BlockSpec(memory_space=pltpu.VMEM),
        scratch_shapes=[
            pltpu.VMEM((chips, rows, width), blocks.dtype),
            pltpu.VMEM((chips, rows, width), blocks.dtype),
            pltpu.VMEM((2, chips // 2, rows, width), blocks.dtype),
            dma((chips,)),
            dma((chips,)),
            dma((chips,)),
            dma((2, steps)),
            dma((2, steps)),
        ],
        compiler_params=pltpu.CompilerParams(
            collective_id=7, has_side_effects=True, vmem_limit_bytes=buffers + 2 * 1024 * 1024
        ),
        cost_estimate=pl.CostEstimate(
            flops=20_000_000_000, bytes_accessed=20_000_000, transcendentals=0
        ),
        name="scatter_sum",
    )(blocks)


def from_groups(make):
    groups = lax.axis_size("token")
    mine = lax.axis_index("token")
    taken = [make(mine)]
    for shift in range(1, groups):
        pairs = [(t, (t + shift) % groups) for t in range(groups)]
        taken.append(lax.ppermute(make((mine + shift) % groups), "token", pairs))
    return jnp.stack(taken)


def pick(sel, rows):
    return lax.dot_general(
        sel, rows, (((2,), (1,)), ((0,), (0,))), preferred_element_type=jnp.float32
    ).astype(jnp.bfloat16)


def transpose_jacobian(everyone, sel, slot_gate, slopes, up_weight, down_weight):
    blocks, capacity, rows = sel.shape
    picked = pick(sel, everyone).reshape(blocks * capacity, -1)
    inner_prod = jnp.dot(picked, down_weight, preferred_element_type=jnp.float32)
    scaled = (inner_prod * slopes).astype(jnp.bfloat16)
    pieces = lax.dot_general(
        scaled, up_weight, (((1,), (1,)), ((), ())), preferred_element_type=jnp.float32
    ).astype(jnp.bfloat16)
    weighted = (pieces.astype(jnp.float32) * slot_gate.reshape(-1, 1)).astype(jnp.bfloat16)
    spread = lax.dot_general(
        sel,
        weighted.reshape(blocks, capacity, -1),
        (((1,), (1,)), ((0,), (0,))),
        preferred_element_type=jnp.float32,
    ).astype(jnp.bfloat16)
    return scatter_sum(spread)


def body(cotangent, expert_ids, gate_values, hidden_pre, up_weight, down_weight):
    experts = lax.axis_size("expert")
    groups = lax.axis_size("token")
    rows, width = cotangent.shape
    top = expert_ids.shape[1]
    padded = -(-2 * top // 16) * 16
    routes = jnp.concatenate([expert_ids.T.astype(jnp.float32), gate_values.T], axis=0)
    routes = jnp.pad(routes, ((0, padded - 2 * top), (0, 0)))
    routes = from_groups(lambda group: routes).reshape(groups * padded, rows)
    everyone, all_routes, slopes, active = gather_rows([cotangent, routes], 1, [hidden_pre[0]])
    capacity = slopes.shape[0] // experts
    acts = from_groups(lambda group: active)
    all_routes = all_routes.reshape(experts * groups, padded, rows).transpose(0, 2, 1)
    all_sel, all_gate = slot_tables(
        all_routes[:, :, :top].astype(jnp.int32), all_routes[:, :, top : 2 * top], capacity
    )
    by_group = all_sel.reshape(experts, groups, capacity, rows)
    sel = by_group[:, 0]
    slot_gate = all_gate.reshape(experts, groups, capacity)[:, 0]
    first_term = transpose_jacobian(
        everyone, sel, slot_gate, slopes, up_weight[0], down_weight[0]
    )
    (everyone,) = gather_rows([first_term], 2)
    second = transpose_jacobian(everyone, sel, slot_gate, slopes, up_weight[0], down_weight[0])
    input_grad = (
        cotangent.astype(jnp.float32) + first_term.astype(jnp.float32) + second.astype(jnp.float32)
    ).astype(jnp.bfloat16)
    share = width // groups
    columns = from_groups(
        lambda group: lax.dynamic_slice_in_dim(input_grad, group * share, share, 1)
    ).reshape(groups * rows, share)
    (everyone,) = gather_rows([columns], 3)
    everyone = everyone.reshape(experts * groups, rows, share)
    picked = pick(all_sel, everyone)
    routed = (picked.astype(jnp.float32) * all_gate[:, :, None]).astype(jnp.bfloat16)
    acts = acts.reshape(groups, experts, capacity, -1).transpose(1, 0, 2, 3)
    summed = lax.dot_general(
        routed.reshape(experts * groups * capacity, -1),
        acts.reshape(experts * groups * capacity, -1),
        (((0,), (0,)), ((), ())),
        preferred_element_type=jnp.float32,
    )
    grad_out = (summed * grad_scale).astype(jnp.bfloat16)[None]
    return (input_grad, grad_out)


def solution(mesh):
    in_specs = (
        P(("expert", "token"), None),
        P(("expert", "token"), None),
        P(("expert", "token"), None),
        P("expert", "token", None),
        P("expert", None, None),
        P("expert", None, None),
    )
    out_specs = (P(("expert", "token"), None), P("expert", "token", None))
    return jax.shard_map(body, mesh=mesh, in_specs=in_specs, out_specs=out_specs, check_vma=False)
```
